32 devices in a mesh: member: 8 (over y, x, core), dp: 4 (over z).
Axes of the slice: x: 2, y: 2, z: 4, core: 2. Of those that a mesh axis runs over, the one named last changes fastest.
Arguments:
- trunk: bfloat16 [1576, 1024], P('dp'), may hold values from -6 to 6
- normgain: float32 [1024], replicated, may hold values from 0.25 to 1.75
- expand: bfloat16 [1024, 2048], P('member'), may hold values from -0.1875 to 0.1875
- shrink: bfloat16 [2048, 1024], P('member'), may hold values from -0.125 to 0.125
- inscale: float32 [8, 1024], P('member'), may hold values from 0.25 to 1.75
- hidscale: float32 [8, 2048], P('member'), may hold values from 0.25 to 1.75
- actscale: float32 [8, 2048], P('member'), may hold values from 0.25 to 1.75
- outscale: float32 [8, 1024], P('member'), may hold values from 0.25 to 1.75
- cotangent: bfloat16 [8, 1576, 1024], P('member', 'dp'), may hold values from -6 to 6
Outputs:
- trunk_grad: bfloat16 [1576, 1024], P('dp', 'member')
- expand_grad: float32 [1024, 2048], P('member')
- shrink_grad: float32 [2048, 1024], P('member')
- inscale_grad: float32 [8, 1024], P('member')
- hidscale_grad: float32 [8, 2048], P('member')
- actscale_grad: float32 [8, 2048], P('member')
- outscale_grad: float32 [8, 1024], P('member')
- normgain_grad: float32 [1024], replicated
The draws below stay inside these ranges and needn't reach their ends.
All inputs are finite; a program needn't handle non-finite values.
Results may differ from the reference program's by a relative error of at most 0.024.
Values may be sent and summed in bfloat16 or wider, within the bound.
No kernel may reach another device: no remote copies, remote signals or barrier semaphores. Data moves between devices by JAX's collectives and lax.ppermute only.
A program may use at most 64 MiB of HBM per device.

```python
import jax
import jax.numpy as jnp
from jax import lax

D = 1024
FF = 2048
TOK_DEV = 394
TOKENS = 1576
MEMBERS = 8
N_DP = 4


def with_spikes(result, rng, source, target, parts, factor):
    owner, partner = [(jnp.arange(result.shape[axis_at]) // (result.shape[axis_at] // parts)).reshape([-1 if axis == axis_at else 1 for axis in range(result.ndim)]) for axis_at in (source, target)]
    chosen = jax.random.permutation(rng, parts)[partner]
    strong = (owner == chosen) | (owner == (partner + parts // 2) % parts)
    return jnp.where(strong, factor * result, result)


def level_of(rng, dims, cuts, least, high):
    level = 1.0
    for dim, parts in cuts:
        heights = jax.random.uniform(jax.random.fold_in(jax.random.fold_in(rng, 6), dim), (parts,), jnp.float32, least / len(cuts), high / len(cuts))
        level = level * jnp.repeat(jnp.exp(heights), dims[dim] // parts).reshape((-1,) + (1,) * (len(dims) - 1 - dim))
    return level


def centred(rng, shape, scale, bound, shards=(), kind=jnp.bfloat16):
    drawn = scale * jax.random.normal(rng, shape, jnp.float32)
    if shards:
        drawn = drawn * level_of(rng, shape, shards, -0.22, 0.18)
    return jnp.clip(drawn, -bound, bound).astype(kind)


def heavy_noise(key, dims, spread, reach, cuts, heavy, kind=jnp.bfloat16):
    values = spread * jax.random.normal(key, dims, jnp.float32)
    if cuts:
        values = values * level_of(key, dims, cuts, -0.22, 0.18)
    return jnp.clip(with_spikes(values, jax.random.fold_in(key, 3), *heavy), -reach, reach).astype(kind)


def setup_inputs(seed: int = 0) -> dict:
    seeds = jax.random.split(jax.random.key(seed), 10)
    return {
        "trunk": centred(seeds[0], (TOKENS, D), 1.0, 6.0, ((0, 4),)),
        "normgain": jnp.clip(1.0 + 0.15 * jax.random.normal(seeds[1], (D,), jnp.float32), 0.25, 1.75),
        "expand": centred(seeds[2], (D, FF), D ** -0.5, 0.1875, ((0, 8),)),
        "shrink": centred(seeds[3], (FF, D), FF ** -0.5, 0.125, ((0, 8),)),
        "inscale": jnp.clip(1.0 + 0.15 * jax.random.normal(seeds[4], (MEMBERS, D), jnp.float32), 0.25, 1.75),
        "hidscale": jnp.clip(1.0 + 0.15 * jax.random.normal(seeds[5], (MEMBERS, FF), jnp.float32), 0.25, 1.75),
        "actscale": jnp.clip(1.0 + 0.15 * jax.random.normal(seeds[6], (MEMBERS, FF), jnp.float32), 0.25, 1.75),
        "outscale": jnp.clip(1.0 + 0.15 * jax.random.normal(seeds[7], (MEMBERS, D), jnp.float32), 0.25, 1.75),
        "cotangent": heavy_noise(seeds[8], (MEMBERS, TOKENS, D), 1.0, 6.0, ((0, 8), (1, 4)), (0, 2, 8, 2.0)),
    }


eps = 1e-06
coeff = 0.7978845608028654

def gelu_pair(hidden):
    inner = coeff * (hidden + 0.044715 * hidden * hidden * hidden)
    tangent = jnp.tanh(inner)
    active = 0.5 * hidden * (1.0 + tangent)
    slope = 0.5 * (1.0 + tangent) + 0.5 * hidden * (1.0 - tangent * tangent) * coeff * (1.0 + 3.0 * 0.044715 * hidden * hidden)
    return (active, slope)

def block_terms(left, right):
    left_blocks = left.astype(jnp.float32).reshape(N_DP, TOK_DEV, left.shape[1])
    right_blocks = right.astype(jnp.float32).reshape(N_DP, TOK_DEV, right.shape[1])
    terms = jnp.einsum('bti,btj->bij', left_blocks, right_blocks, precision=lax.Precision.HIGHEST)
    rounded = lax.optimization_barrier(terms.astype(jnp.bfloat16))
    return lax.optimization_barrier(jnp.sum(rounded.astype(jnp.float32), axis=0))

def reference(trunk, normgain, expand, shrink, inscale, hidscale, actscale, outscale, cotangent):
    tokens = trunk.astype(jnp.float32)
    centered = tokens - lax.optimization_barrier(jnp.mean(tokens, axis=1, keepdims=True))
    variance = lax.optimization_barrier(jnp.mean(centered * centered, axis=1, keepdims=True))
    inv_std = lax.rsqrt(variance + eps)
    normed = centered * inv_std
    gained = normed * normgain

    def member_step(carry, pieces):
        trunk_acc, expand_acc, shrink_acc, gain_acc = carry
        scale_in, scale_hid, scale_act, scale_out, cot = pieces
        scaled_in = (gained * scale_in).astype(jnp.bfloat16)
        project = jnp.dot(scaled_in, expand, preferred_element_type=jnp.float32)
        hidden = project * scale_hid
        active, slope = gelu_pair(hidden)
        scaled_act = (active * scale_act).astype(jnp.bfloat16)
        second = jnp.dot(scaled_act, shrink, preferred_element_type=jnp.float32)
        upstream = cot.astype(jnp.float32)
        grad_out = lax.optimization_barrier(jnp.sum(upstream * second, axis=0))
        scaled_cot = (upstream * scale_out).astype(jnp.bfloat16)
        back_act = jnp.dot(scaled_cot, shrink.T, preferred_element_type=jnp.float32)
        grad_act = lax.optimization_barrier(jnp.sum(back_act * active, axis=0))
        back_hidden = back_act * scale_act * slope
        grad_hid = lax.optimization_barrier(jnp.sum(back_hidden * project, axis=0))
        back_proj = (back_hidden * scale_hid).astype(jnp.bfloat16)
        shrink_acc = shrink_acc + block_terms(scaled_act, scaled_cot)
        expand_acc = expand_acc + block_terms(scaled_in, back_proj)
        back_norm = jnp.dot(back_proj, expand.T, preferred_element_type=jnp.float32)
        grad_in = lax.optimization_barrier(jnp.sum(back_norm * gained, axis=0))
        back_scaled = back_norm * scale_in
        gain_acc = gain_acc + lax.optimization_barrier(jnp.sum(back_scaled * normed, axis=0))
        back_unit = back_scaled * normgain
        back_trunk = inv_std * (back_unit - lax.optimization_barrier(jnp.mean(back_unit, axis=1, keepdims=True)) - normed * lax.optimization_barrier(jnp.mean(back_unit * normed, axis=1, keepdims=True)))
        trunk_acc = trunk_acc + upstream + back_trunk
        return ((trunk_acc, expand_acc, shrink_acc, gain_acc), (grad_in, grad_hid, grad_act, grad_out))
    start = (jnp.zeros(tokens.shape, jnp.float32), jnp.zeros(expand.shape, jnp.float32), jnp.zeros(shrink.shape, jnp.float32), jnp.zeros(normgain.shape, jnp.float32))
    carry, grads = lax.scan(member_step, start, (inscale, hidscale, actscale, outscale, cotangent))
    trunk_acc, expand_acc, shrink_acc, gain_acc = carry
    grad_in, grad_hid, grad_act, grad_out = grads
    return (trunk_acc.astype(jnp.bfloat16), expand_acc, shrink_acc, grad_in, grad_hid, grad_act, grad_out, gain_acc)
```

```python
import jax
import jax.numpy as jnp
from jax import lax
from jax.sharding import PartitionSpec as P

eps = 1e-06
coeff = 0.7978845608028654
f32 = jnp.float32
bf16 = jnp.bfloat16


def gelu_pair(hidden):
    inner = coeff * (hidden + 0.044715 * hidden * hidden * hidden)
    tangent = jnp.tanh(inner)
    active = 0.5 * hidden * (1.0 + tangent)
    slope = 0.5 * (1.0 + tangent) + 0.5 * hidden * (1.0 - tangent * tangent) * coeff * (
        1.0 + 3.0 * 0.044715 * hidden * hidden
    )
    return (active, slope)


def dot(left, right, contract):
    return lax.dot_general(left, right, ((contract[:1], contract[1:]), ((), ())), preferred_element_type=f32)


def tree_sum(terms):
    terms = list(terms)
    while len(terms) > 1:
        terms = [terms[i] + terms[i + 1] for i in range(0, len(terms), 2)]
    return terms[0]


def sum_over_dp(chunks, count):
    if count != 4:
        return [lax.psum(chunk, "dp").astype(f32) for chunk in chunks]
    place = lax.axis_index("dp")
    end = (place == 0) | (place == 3)
    inward = [lax.ppermute(c, "dp", [(0, 1), (3, 2)]) for c in chunks]
    halves = [(a.astype(f32) + b.astype(f32)).astype(bf16) for a, b in zip(chunks, inward)]
    across = [lax.ppermute(h, "dp", [(1, 2), (2, 1)]) for h in halves]
    totals = [(a.astype(f32) + b.astype(f32)).astype(bf16) for a, b in zip(halves, across)]
    outward = [lax.ppermute(t, "dp", [(1, 0), (2, 3)]) for t in totals]
    return [jnp.where(end, o, lax.reduce_precision(t, 8, 7)).astype(f32) for t, o in zip(totals, outward)]


def small_sum_over_dp(value, count):
    if count & (count - 1):
        return lax.psum(value, "dp")
    parts = [value] + [
        lax.ppermute(value, "dp", [(i, i ^ r) for i in range(count)]) for r in range(1, count)
    ]
    return tree_sum(parts)


def make_body(members, count):
    chips = members // 2
    slots = range(chips)

    def swap(value, mask):
        return lax.ppermute(value, "member", [(i, i ^ mask) for i in range(members)])

    def body(trunk, normgain, expand, shrink, inscale, hidscale, actscale, outscale, cotangent):
        index = lax.axis_index("member")
        chip, core = index // 2, index % 2
        tok, width = trunk.shape
        rows = expand.shape[0]
        ff = expand.shape[1]
        quarter = ff // chips

        scales = jnp.concatenate([inscale[0], hidscale[0], actscale[0]])
        scale_of = [scales] + [swap(scales, 2 * r) for r in slots[1:]]
        piece_of = [
            lax.dynamic_slice(expand, (0, (chip ^ r) * quarter), (rows, quarter)) for r in slots
        ]
        piece_of = [piece_of[0]] + [swap(piece_of[r], 2 * r) for r in slots[1:]]
        shrink_other = swap(shrink, 1)
        pieces = jnp.stack(piece_of)
        pieces = jnp.concatenate([pieces, swap(pieces, 1)])
        expand_q = jnp.concatenate(
            [
                lax.dynamic_index_in_dim(pieces, (c ^ core) * chips + (p ^ chip), 0, keepdims=False)
                for p in range(chips)
                for c in range(2)
            ]
        )
        first = core == 0
        shrink_q = jnp.concatenate(
            [jnp.where(first, shrink, shrink_other), jnp.where(first, shrink_other, shrink)]
        )

        upstream = cotangent[0].astype(f32)
        scaled_cot = (upstream * outscale[0]).astype(bf16)
        if chips == 4:
            by_x, by_y = swap(scaled_cot, 2), swap(scaled_cot, 4)
            half = width // 2
            corner = jnp.concatenate([swap(by_y[:, :half], 2), swap(by_x[:, half:], 4)], axis=1)
            cot_of = [scaled_cot, by_x, by_y, corner]
        else:
            cot_of = [scaled_cot] + [swap(scaled_cot, 2 * r) for r in slots[1:]]

        tokens = trunk.astype(f32)
        centered = tokens - jnp.mean(tokens, axis=1, keepdims=True)
        variance = jnp.mean(centered * centered, axis=1, keepdims=True)
        inv_std = lax.rsqrt(variance + eps)
        normed = centered * inv_std
        gained = normed * normgain

        shrink_acc, expand_acc, unit, packs = 0.0, 0.0, 0.0, []
        gain_part = 0.0
        for r in slots:
            scale_in = scale_of[r][:width]
            scale_hid = lax.dynamic_slice(scale_of[r], (width + chip * quarter,), (quarter,))
            scale_act = lax.dynamic_slice(scale_of[r], (width + ff + chip * quarter,), (quarter,))
            scaled_in = (gained * scale_in).astype(bf16)
            project = dot(scaled_in, expand_q, (1, 0))
            active, slope = gelu_pair(project * scale_hid)
            scaled_act = (active * scale_act).astype(bf16)
            back_act = dot(cot_of[r], shrink_q, (1, 1))
            grad_act = jnp.sum(back_act * active, axis=0)
            back_hidden = back_act * scale_act * slope
            grad_hid = jnp.sum(back_hidden * project, axis=0)
            back_proj = (back_hidden * scale_hid).astype(bf16)
            shrink_term = dot(scaled_act, cot_of[r], (0, 0))
            grad_out = jnp.sum(shrink_term * shrink_q.astype(f32), axis=0)
            shrink_acc = shrink_acc + shrink_term
            expand_acc = expand_acc + dot(scaled_in, back_proj, (0, 0))
            back_norm = dot(back_proj, expand_q, (1, 1))
            grad_in = jnp.sum(back_norm * normed, axis=0)
            gain_part = gain_part + grad_in * scale_in
            unit = unit + back_norm * scale_in
            packs.append(jnp.concatenate([grad_in, grad_out, grad_hid, grad_act]))

        shrink_rows = shrink.shape[0]
        halves = shrink_acc.astype(bf16).reshape(2, shrink_rows, width)
        mine = lax.dynamic_index_in_dim(halves, core, 0, keepdims=False)
        theirs = swap(lax.dynamic_index_in_dim(halves, 1 - core, 0, keepdims=False), 1)
        shrink_part = (mine.astype(f32) + theirs.astype(f32)).astype(bf16)

        blocks = expand_acc.astype(bf16).reshape(chips, 2, rows, quarter)
        mine = lax.dynamic_index_in_dim(blocks, core, 1, keepdims=False)
        theirs = swap(lax.dynamic_index_in_dim(blocks, 1 - core, 1, keepdims=False), 1)
        blocks = (mine.astype(f32) + theirs.astype(f32)).astype(bf16)
        got = [lax.dynamic_index_in_dim(blocks, chip ^ r, 0, keepdims=False) for r in slots]
        got = jnp.stack([got[0]] + [swap(got[r], 2 * r) for r in slots[1:]])
        expand_part = jnp.concatenate(
            [lax.dynamic_index_in_dim(got, p ^ chip, 0, keepdims=False) for p in range(chips)], axis=1
        )

        cut_s, cut_e = shrink_rows // 2, rows // 2
        sums = sum_over_dp(
            [shrink_part[:cut_s], shrink_part[cut_s:], expand_part[:cut_e], expand_part[cut_e:]], count
        )
        shrink_grad = jnp.concatenate(sums[:2])
        expand_grad = jnp.concatenate(sums[2:])

        unit = unit * normgain
        term = upstream + inv_std * (
            unit
            - jnp.mean(unit, axis=1, keepdims=True)
            - normed * jnp.mean(unit * normed, axis=1, keepdims=True)
        )
        lanes = width // members
        term = term.astype(bf16).reshape(tok, chips, 2, lanes)
        mine = lax.dynamic_index_in_dim(term, core, 2, keepdims=False)
        theirs = swap(lax.dynamic_index_in_dim(term, 1 - core, 2, keepdims=False), 1)
        term = (mine.astype(f32) + theirs.astype(f32)).astype(bf16)
        got = [lax.dynamic_index_in_dim(term, chip ^ r, 1, keepdims=False) for r in slots]
        got = [got[0]] + [swap(got[r], 2 * r) for r in slots[1:]]
        trunk_grad = tree_sum([g.astype(f32) for g in got]).astype(bf16)

        gain_part = gain_part + swap(gain_part, 1)
        packs = [jnp.concatenate([p, gain_part]) for p in packs]
        packs = [packs[0]] + [swap(packs[r], 2 * r) for r in slots[1:]]
        grad_in = tree_sum([p[:width] for p in packs])
        grad_out = tree_sum([p[width : 2 * width] for p in packs])
        gain = tree_sum([p[2 * width + 2 * quarter :] for p in packs])
        inner = jnp.stack([p[2 * width : 2 * width + 2 * quarter] for p in packs])
        inner = [lax.dynamic_index_in_dim(inner, p ^ chip, 0, keepdims=False) for p in range(chips)]
        small = jnp.concatenate(
            [grad_in, grad_out, gain] + [i[:quarter] for i in inner] + [i[quarter:] for i in inner]
        )
        small = small_sum_over_dp(small, count)
        grad_in = small[:width] * normgain
        grad_out = small[width : 2 * width] / outscale[0]
        gain = small[2 * width : 3 * width]
        grad_hid = small[3 * width : 3 * width + ff]
        grad_act = small[3 * width + ff :]
        return (
            trunk_grad,
            expand_grad,
            shrink_grad,
            grad_in[None],
            grad_hid[None],
            grad_act[None],
            grad_out[None],
            gain,
        )

    return body


def solution(mesh):
    return jax.shard_map(
        make_body(mesh.shape["member"], mesh.shape["dp"]),
        mesh=mesh,
        in_specs=(
            P("dp", None),
            P(),
            P("member", None),
            P("member", None),
            P("member", None),
            P("member", None),
            P("member", None),
            P("member", None),
            P("member", "dp", None),
        ),
        out_specs=(
            P("dp", "member"),
            P("member", None),
            P("member", None),
            P("member", None),
            P("member", None),
            P("member", None),
            P("member", None),
            P(),
        ),
        check_vma=False,
    )
```

```python
import jax
import jax.numpy as jnp
from jax import lax
from jax.sharding import PartitionSpec as P

eps = 1e-06
coeff = 0.7978845608028654
f32 = jnp.float32
bf16 = jnp.bfloat16


def gelu_pair(hidden):
    inner = coeff * (hidden + 0.044715 * hidden * hidden * hidden)
    tangent = jnp.tanh(inner)
    active = 0.5 * hidden * (1.0 + tangent)
    slope = 0.5 * (1.0 + tangent) + 0.5 * hidden * (1.0 - tangent * tangent) * coeff * (
        1.0 + 3.0 * 0.044715 * hidden * hidden
    )
    return (active, slope)


def dot(left, right, contract):
    return lax.dot_general(left, right, ((contract[:1], contract[1:]), ((), ())), preferred_element_type=f32)


def tree_sum(terms):
    terms = list(terms)
    while len(terms) > 1:
        terms = [terms[i] + terms[i + 1] for i in range(0, len(terms), 2)]
    return terms[0]


def two_terms(value):
    high = lax.reduce_precision(value, 8, 7)
    return high.astype(bf16), (value - high).astype(bf16)


def one_value(high, low):
    return high.astype(f32) + low.astype(f32)


def add(a, b):
    return a.astype(f32) + b.astype(f32)


def sum_over_dp(chunks, count):
    if count != 4:
        return [lax.psum(chunk, "dp") for chunk in chunks]
    place = lax.axis_index("dp")
    end = (place == 0) | (place == 3)

    def hop(value, pairs):
        return lax.ppermute(value, "dp", pairs)

    inward = [hop(c, [(0, 1), (3, 2)]) for c in chunks]
    halves = []
    for a, b in zip(chunks, inward):
        halves.append(add(a, b).astype(bf16))
    across = [hop(h, [(1, 2), (2, 1)]) for h in halves]
    totals = []
    for a, b in zip(halves, across):
        totals.append(lax.reduce_precision(add(a, b), 8, 7).astype(bf16))
    outward = [hop(t, [(1, 0), (2, 3)]) for t in totals]
    return [jnp.where(end, o, t) for t, o in zip(totals, outward)]


def make_body(members, count):
    chips = members // 2
    slots = range(chips)

    def swap(value, mask):
        return lax.ppermute(value, "member", [(i, i ^ mask) for i in range(members)])

    def body(trunk, normgain, expand, shrink, inscale, hidscale, actscale, outscale, cotangent):
        index = lax.axis_index("member")
        chip, core = index // 2, index % 2
        tok, width = trunk.shape
        rows, ff = expand.shape
        quarter = ff // chips
        lanes = width // members
        shrink_rows = shrink.shape[0]
        first = core == 0

        def outgoing(r):
            at = (chip ^ r) * quarter
            piece = lax.dynamic_slice(expand, (0, at), (rows, quarter))
            factors = jnp.concatenate(
                [
                    inscale.reshape(-1, quarter),
                    lax.dynamic_slice(hidscale, (0, at), (1, quarter)),
                    lax.dynamic_slice(actscale, (0, at), (1, quarter)),
                ]
            )
            return piece, factors

        piece_of, factors_of = [], []
        lines = width // quarter + 2
        for r in slots:
            piece, factors = outgoing(r)
            if r:
                sent = jnp.concatenate([piece, *two_terms(factors)])
            if r:
                got = swap(sent, 2 * r)
                piece = got[:rows]
                factors = one_value(got[rows : rows + lines], got[rows + lines :])
            piece_of.append(piece)
            factors_of.append(factors)
        shrink_other = swap(shrink, 1)

        upstream = cotangent[0].astype(f32)
        scaled_cot = (upstream * outscale[0]).astype(bf16)
        if chips == 4:
            half = width // 2
            by_x, by_y = swap(scaled_cot, 2), swap(scaled_cot, 4)
            left, right = by_y[:, :half], by_x[:, half:]
            left, right = swap(left, 2), swap(right, 4)
            corner = jnp.concatenate([left, right], axis=1)
            cot_of = [scaled_cot, by_x, by_y, corner]
        else:
            cot_of = [scaled_cot] + [swap(scaled_cot, 2 * r) for r in slots[1:]]

        pieces = jnp.stack(piece_of)
        pieces_other = swap(pieces, 1)
        pieces = jnp.concatenate([pieces, pieces_other])
        expand_q = jnp.concatenate(
            [
                lax.dynamic_index_in_dim(pieces, (c ^ core) * chips + (p ^ chip), 0, keepdims=False)
                for p in range(chips)
                for c in range(2)
            ]
        )
        shrink_q = jnp.concatenate(
            [jnp.where(first, shrink, shrink_other), jnp.where(first, shrink_other, shrink)]
        )
        tokens = trunk.astype(f32)
        centered = tokens - jnp.mean(tokens, axis=1, keepdims=True)
        variance = jnp.mean(centered * centered, axis=1, keepdims=True)
        inv_std = lax.rsqrt(variance + eps)
        normed = centered * inv_std
        gained = normed * normgain

        forward = []
        for r in slots:
            scale_in = factors_of[r][: lines - 2].reshape(-1)
            scaled_in = (gained * scale_in).astype(bf16)
            forward.append((scale_in, scaled_in, dot(scaled_in, expand_q, (1, 0))))

        shrink_acc, expand_acc, unit, packs = 0.0, 0.0, 0.0, []
        gain_part = 0.0
        for r in slots:
            scale_in, scaled_in, project = forward[r]
            scale_hid, scale_act = factors_of[r][lines - 2], factors_of[r][lines - 1]
            active, slope = gelu_pair(project * scale_hid)
            scaled_act = (active * scale_act).astype(bf16)
            shrink_term = dot(scaled_act, cot_of[r], (0, 0))
            grad_out = jnp.sum(shrink_term * shrink_q.astype(f32), axis=0)
            shrink_acc = shrink_acc + shrink_term
            back_act = dot(cot_of[r], shrink_q, (1, 1))
            grad_act = jnp.sum(back_act * active, axis=0)
            back_hidden = back_act * scale_act * slope
            grad_hid = jnp.sum(back_hidden * project, axis=0)
            back_proj = (back_hidden * scale_hid).astype(bf16)
            expand_acc = expand_acc + dot(scaled_in, back_proj, (0, 0))
            back_norm = dot(back_proj, expand_q, (1, 1))
            grad_in = jnp.sum(back_norm * normed, axis=0)
            gain_part = gain_part + grad_in * scale_in
            unit = unit + back_norm * scale_in
            packs.append((grad_in, grad_out, grad_hid, grad_act))
            if r in (0, chips - 2):
                shrink_acc, expand_acc, unit, gain_part, packs = lax.optimization_barrier(
                    (shrink_acc, expand_acc, unit, gain_part, packs)
                )

        mine = shrink_acc.astype(bf16)
        theirs = swap(mine, 1)
        chunks = []
        for k in range(2):
            at = core * shrink_rows + k * (shrink_rows // 2)
            size = (shrink_rows // 2, width)
            chunks.append(
                add(lax.dynamic_slice(mine, (at, 0), size), lax.dynamic_slice(theirs, (at, 0), size)).astype(bf16)
            )

        mine = expand_acc.astype(bf16)
        theirs = swap(mine, 1)
        got = []
        for r in slots:
            at = (2 * (chip ^ r) + core) * rows
            size = (rows, quarter)
            block = add(lax.dynamic_slice(mine, (at, 0), size), lax.dynamic_slice(theirs, (at, 0), size)).astype(bf16)
            got.append(swap(block, 2 * r) if r else block)
        got = jnp.stack(got)
        expand_part = jnp.concatenate(
            [lax.dynamic_index_in_dim(got, p ^ chip, 0, keepdims=False) for p in range(chips)], axis=1
        )
        cut = rows // 2
        chunks.append(expand_part[:cut])

        unit = unit * normgain
        term = upstream + inv_std * (
            unit
            - jnp.mean(unit, axis=1, keepdims=True)
            - normed * jnp.mean(unit * normed, axis=1, keepdims=True)
        )
        gain_terms = two_terms(gain_part.reshape(1, width))
        mine = jnp.concatenate([*gain_terms, jnp.zeros((14, width), bf16), term.astype(bf16)])
        theirs = swap(mine, 1)
        gain_part = one_value(*gain_terms) + one_value(theirs[:1], theirs[1:2])
        gain_terms = two_terms(gain_part.reshape(-1, lanes))
        depth = width // lanes
        inner = 2 * quarter // lanes
        got = []
        for r in slots:
            at = (2 * (chip ^ r) + core) * lanes
            block = add(
                lax.dynamic_slice(mine[16:], (0, at), (tok, lanes)),
                lax.dynamic_slice(theirs[16:], (0, at), (tok, lanes)),
            ).astype(bf16)
            pack = two_terms(jnp.concatenate(packs[r]).reshape(-1, lanes))
            pack = jnp.concatenate([pack[0], gain_terms[0], pack[1], gain_terms[1]])
            block = jnp.concatenate([pack, block])
            got.append(swap(block, 2 * r) if r else block)
        size = 3 * depth + inner
        trunk_grad = tree_sum([g[2 * size :].astype(f32) for g in got]).astype(bf16)

        got = [one_value(g[:size], g[size : 2 * size]) for g in got]
        ends = tree_sum([jnp.concatenate([g[: 2 * depth], g[2 * depth + inner :]]) for g in got])
        inside = jnp.stack([g[2 * depth : 2 * depth + inner] for g in got])
        inside = [lax.dynamic_index_in_dim(inside, p ^ chip, 0, keepdims=False) for p in range(chips)]
        small = jnp.concatenate(
            [ends] + [i[: inner // 2] for i in inside] + [i[inner // 2 :] for i in inside]
        ).reshape(-1)
        used = small.shape[0]
        lines = -(-used // ff)
        small = jnp.pad(small, (0, lines * ff - used)).reshape(lines, ff).astype(bf16)
        chunks.append(jnp.concatenate([expand_part[cut:], small]))

        sums = sum_over_dp(chunks, count)
        shrink_grad = jnp.concatenate(sums[:2]).astype(f32)
        expand_grad = jnp.concatenate([sums[2], sums[3][: rows - cut]]).astype(f32)
        small = sums[3][rows - cut :].astype(f32).reshape(-1)
        grad_in = small[:width] * normgain
        grad_out = small[width : 2 * width] / outscale[0]
        gain = small[2 * width : 3 * width]
        grad_hid = small[3 * width : 3 * width + ff]
        grad_act = small[3 * width + ff : used]
        return (
            trunk_grad,
            expand_grad,
            shrink_grad,
            grad_in[None],
            grad_hid[None],
            grad_act[None],
            grad_out[None],
            gain,
        )

    return body


def solution(mesh):
    return jax.shard_map(
        make_body(mesh.shape["member"], mesh.shape["dp"]),
        mesh=mesh,
        in_specs=(
            P("dp", None),
            P(),
            P("member", None),
            P("member", None),
            P("member", None),
            P("member", None),
            P("member", None),
            P("member", None),
            P("member", "dp", None),
        ),
        out_specs=(
            P("dp", "member"),
            P("member", None),
            P("member", None),
            P("member", None),
            P("member", None),
            P("member", None),
            P("member", None),
            P(),
        ),
        check_vma=False,
    )
```
